512 devices in a mesh: dp: 64 (over y, z), mp: 8 (over x, core).
Axes of the slice: x: 4, y: 8, z: 8, core: 2. Of those that a mesh axis runs over, the one named last changes fastest.
Arguments:
- hidden: bfloat16 [8192, 4096], P('dp', 'mp'), may hold values from -6 to 6
- attended: bfloat16 [8192, 4096], P('dp', 'mp'), may hold values from -6 to 6
- query_cotangent: bfloat16 [8192, 4096], P('dp', 'mp'), may hold values from -1.5 to 1.5
- output_cotangent: bfloat16 [8192, 4096], P('dp', 'mp'), may hold values from -1.5 to 1.5
- query_projection_weight: bfloat16 [4096, 4096], P('dp', 'mp'), may hold values from -0.09375 to 0.09375
- output_projection_weight: bfloat16 [4096, 4096], P('dp', 'mp'), may hold values from -0.09375 to 0.09375
- narrower: bfloat16 [1024, 16, 4096], P('dp', None, 'mp'), may hold values from -0.09375 to 0.09375
- widener: bfloat16 [1024, 16, 4096], P('dp', None, 'mp'), may hold values from -0.375 to 0.375
- reducer: bfloat16 [1024, 16, 4096], P('dp', None, 'mp'), may hold values from -0.09375 to 0.09375
- enlarger: bfloat16 [1024, 16, 4096], P('dp', None, 'mp'), may hold values from -0.375 to 0.375
- block_adapter: int32 [2048], P('dp'), may hold values from 0 to 1023, as said below
- block_fill: int32 [2048], P('dp'), may hold values from 1 to 4
Outputs:
- queries: bfloat16 [8192, 4096], P('dp', 'mp')
- projected: bfloat16 [8192, 4096], P('dp', 'mp')
- hidden_state_gradient: bfloat16 [8192, 4096], P('dp', 'mp')
- attention_output_gradient: bfloat16 [8192, 4096], P('dp', 'mp')
- narrower_gradient: float32 [1024, 16, 4096], P('dp', None, 'mp')
- widener_gradient: float32 [1024, 16, 4096], P('dp', None, 'mp')
- reducer_gradient: float32 [1024, 16, 4096], P('dp', None, 'mp')
- enlarger_gradient: float32 [1024, 16, 4096], P('dp', None, 'mp')
The draws below stay inside these ranges and needn't reach their ends.
Inputs may be any that keep to these rules, and one draw needn't show every extreme that they name: `block_adapter`: the owner of adapter e is e // 16. Among the 32 blocks of one group (one index of dp), at most 1 have adapters of one owner, and some owner has exactly 1 block in every group.
All inputs are finite; a program needn't handle non-finite values.
Results may differ from the reference program's by a relative error of at most 0.015.
Values may be sent and summed in bfloat16 or wider, within the bound.
No kernel may reach another device: no remote copies, remote signals or barrier semaphores. Data moves between devices by JAX's collectives and lax.ppermute only.
A program may use at most 64 MiB of HBM per device.

```python
import jax
import jax.numpy as jnp
from jax import lax

MODEL_FEATURES = 4096
QUERY_FEATURES = 4096
RANK = 16
ADP_DEV = 16
GROUP_TOKENS = 128
BLOCK = 4
TOKEN_SLOTS = 8192
ADAPTERS = 1024
BLOCKS = 2048
N_DP = 64
N_MP = 8


def draw_block_adapter(key, part):
    groups = ADAPTERS // ADP_DEV
    per_group = GROUP_TOKENS // BLOCK
    slots = (per_group + groups - 1) // groups
    hot_key, group_key, local_key = jax.random.split(jax.random.fold_in(key, 7), 3)
    hottest = jax.random.randint(hot_key, (), 0, groups)

    def one_group(group_seed):
        perm_key, order_key = jax.random.split(group_seed)
        entries = jax.random.permutation(perm_key, (groups - 1) * slots)[:per_group - slots]
        others = (entries // slots).astype(jnp.int32)
        others = others + (others >= hottest).astype(jnp.int32)
        owners = jnp.concatenate([jnp.full((slots,), hottest, jnp.int32), others])
        return jax.random.permutation(order_key, owners)
    owners = jax.vmap(one_group)(jax.random.split(group_key, groups))
    local = jax.random.randint(local_key, (groups, per_group), 0, ADP_DEV)
    return (owners * ADP_DEV + local).reshape(-1).astype(jnp.int32)


def touch_ends(array, stream_key, least, top_value):
    dims = array.shape
    index_at = [jax.random.randint(jax.random.fold_in(stream_key, axis), (), 0, dims[axis]) for axis in range(len(dims))]
    array = array.at[tuple(index_at)].set(least)
    longest = dims.index(max(dims))
    index_at[longest] = (index_at[longest] + 1) % dims[longest]
    return array.at[tuple(index_at)].set(top_value)


def level_of(key, dims, cuts, low, largest):
    level = 1.0
    for axis_at, parts in cuts:
        draws = jax.random.uniform(jax.random.fold_in(jax.random.fold_in(key, 6), axis_at), (parts,), jnp.float32, low / len(cuts), largest / len(cuts))
        level = level * jnp.repeat(jnp.exp(draws), dims[axis_at] // parts).reshape((-1,) + (1,) * (len(dims) - 1 - axis_at))
    return level


def gaussian(stream_key, shape, spread, reach, cuts=(), kind=jnp.bfloat16):
    level = level_of(stream_key, shape, cuts, -0.22, 0.18) if cuts else 1.0
    result = jax.random.normal(stream_key, shape, jnp.float32) * spread * level
    return jnp.minimum(jnp.maximum(result, -reach), reach).astype(kind)


def setup_inputs(seed: int = 0) -> dict:
    keys = jax.random.split(jax.random.key(seed), 13)
    return {
        "hidden": gaussian(keys[0], (TOKEN_SLOTS, MODEL_FEATURES), 1.0, 6.0, ((0, 64), (1, 8))),
        "attended": gaussian(keys[1], (TOKEN_SLOTS, QUERY_FEATURES), 1.0, 6.0, ((0, 64), (1, 8))),
        "query_cotangent": gaussian(keys[2], (TOKEN_SLOTS, QUERY_FEATURES), 0.25, 1.5, ((0, 64), (1, 8))),
        "output_cotangent": gaussian(keys[3], (TOKEN_SLOTS, MODEL_FEATURES), 0.25, 1.5, ((0, 64), (1, 8))),
        "query_projection_weight": gaussian(keys[4], (MODEL_FEATURES, QUERY_FEATURES), MODEL_FEATURES ** -0.5, 0.09375, ((0, 64), (1, 8))),
        "output_projection_weight": gaussian(keys[5], (QUERY_FEATURES, MODEL_FEATURES), QUERY_FEATURES ** -0.5, 0.09375, ((0, 64), (1, 8))),
        "narrower": gaussian(keys[6], (ADAPTERS, RANK, MODEL_FEATURES), MODEL_FEATURES ** -0.5, 0.09375, ((0, 64), (2, 8))),
        "widener": gaussian(keys[7], (ADAPTERS, RANK, QUERY_FEATURES), (16 * RANK) ** -0.5, 0.375, ((0, 64), (2, 8))),
        "reducer": gaussian(keys[8], (ADAPTERS, RANK, QUERY_FEATURES), QUERY_FEATURES ** -0.5, 0.09375, ((0, 64), (2, 8))),
        "enlarger": gaussian(keys[9], (ADAPTERS, RANK, MODEL_FEATURES), (16 * RANK) ** -0.5, 0.375, ((0, 64), (2, 8))),
        "block_adapter": draw_block_adapter(jax.random.fold_in(keys[12], 71), 0),
        "block_fill": touch_ends(jax.random.randint(keys[11], (BLOCKS,), 1, BLOCK + 1), jax.random.fold_in(keys[11], 1), 1, BLOCK).astype(jnp.int32),
    }


adapter_scale = 2.0


def batched_result(form, left, right):
    return jnp.einsum(form, left.astype(jnp.float32), right.astype(jnp.float32), precision=lax.Precision.HIGHEST)


def reference(hidden, attended, query_cotangent, output_cotangent, query_projection_weight, output_projection_weight, narrower, widener, reducer, enlarger, block_adapter, block_fill):
    per_group = GROUP_TOKENS // BLOCK
    row_ids = lax.broadcasted_iota(jnp.int32, (BLOCKS, BLOCK), 1)
    live = (row_ids < block_fill[:, None]).astype(jnp.bfloat16).reshape(TOKEN_SLOTS, 1)
    query_masked = query_cotangent * live
    output_masked = output_cotangent * live

    def per_group_work(inputs):
        hid, att, qcot, ocot, ids = inputs
        hidden_block_list = hid.reshape(per_group, BLOCK, MODEL_FEATURES)
        attended_block_list = att.reshape(per_group, BLOCK, QUERY_FEATURES)
        query_cotangent_blocks = qcot.reshape(per_group, BLOCK, QUERY_FEATURES)
        output_cotangent_blocks = ocot.reshape(per_group, BLOCK, MODEL_FEATURES)
        query_down_factor = narrower[ids]
        query_up_factor = widener[ids]
        output_down_factor = reducer[ids]
        output_up_factor = enlarger[ids]
        query_rank_rows = batched_result("brf,bkf->brk", hidden_block_list, query_down_factor).astype(jnp.bfloat16)
        output_rank_rows = batched_result("brf,bkf->brk", attended_block_list, output_down_factor).astype(jnp.bfloat16)
        query_backward_pass = batched_result("brf,bkf->brk", query_cotangent_blocks, query_up_factor).astype(jnp.bfloat16)
        output_backward_pass = batched_result("brf,bkf->brk", output_cotangent_blocks, output_up_factor).astype(jnp.bfloat16)
        query_adapter_term = (adapter_scale * batched_result("ixa,iaq->ixq", query_rank_rows, query_up_factor)).astype(jnp.bfloat16)
        output_adapter_term = (adapter_scale * batched_result("ixa,iaq->ixq", output_rank_rows, output_up_factor)).astype(jnp.bfloat16)
        hidden_adapter_term = (adapter_scale * batched_result("ixa,iaq->ixq", query_backward_pass, query_down_factor)).astype(jnp.bfloat16)
        attended_adapter_term = (adapter_scale * batched_result("ixa,iaq->ixq", output_backward_pass, output_down_factor)).astype(jnp.bfloat16)
        query_down_gradient = adapter_scale * batched_result("iot,iol->itl", query_backward_pass, hidden_block_list)
        query_up_gradient = adapter_scale * batched_result("iot,iol->itl", query_rank_rows, query_cotangent_blocks)
        output_down_gradient = adapter_scale * batched_result("iot,iol->itl", output_backward_pass, attended_block_list)
        output_up_gradient = adapter_scale * batched_result("iot,iol->itl", output_rank_rows, output_cotangent_blocks)
        return (query_adapter_term.reshape(GROUP_TOKENS, QUERY_FEATURES), output_adapter_term.reshape(GROUP_TOKENS, MODEL_FEATURES),
                hidden_adapter_term.reshape(GROUP_TOKENS, MODEL_FEATURES), attended_adapter_term.reshape(GROUP_TOKENS, QUERY_FEATURES),
                query_down_gradient, query_up_gradient, output_down_gradient, output_up_gradient)

    result_list = lax.map(per_group_work, (hidden.reshape(N_DP, GROUP_TOKENS, MODEL_FEATURES), attended.reshape(N_DP, GROUP_TOKENS, QUERY_FEATURES),
                                       query_masked.reshape(N_DP, GROUP_TOKENS, QUERY_FEATURES), output_masked.reshape(N_DP, GROUP_TOKENS, MODEL_FEATURES),
                                       block_adapter.reshape(N_DP, per_group)))
    query_adapter_term = result_list[0].reshape(TOKEN_SLOTS, QUERY_FEATURES)
    output_adapter_term = result_list[1].reshape(TOKEN_SLOTS, MODEL_FEATURES)
    hidden_adapter_term = result_list[2].reshape(TOKEN_SLOTS, MODEL_FEATURES)
    attended_adapter_term = result_list[3].reshape(TOKEN_SLOTS, QUERY_FEATURES)

    def collect(grads, width):
        return jax.ops.segment_sum(grads.reshape(BLOCKS, RANK, width), block_adapter, num_segments=ADAPTERS)

    narrower_gradient = collect(result_list[4], MODEL_FEATURES)
    widener_gradient = collect(result_list[5], QUERY_FEATURES)
    reducer_gradient = collect(result_list[6], QUERY_FEATURES)
    enlarger_gradient = collect(result_list[7], MODEL_FEATURES)

    queries = (jnp.dot(hidden, query_projection_weight, preferred_element_type=jnp.float32) + query_adapter_term.astype(jnp.float32)).astype(jnp.bfloat16)
    projected = (jnp.dot(attended, output_projection_weight, preferred_element_type=jnp.float32) + output_adapter_term.astype(jnp.float32)).astype(jnp.bfloat16)

    query_cols = QUERY_FEATURES // N_MP
    output_cols = MODEL_FEATURES // N_MP
    hidden_total_sum = jnp.zeros((TOKEN_SLOTS, MODEL_FEATURES), jnp.float32)
    attended_total_sum = jnp.zeros((TOKEN_SLOTS, QUERY_FEATURES), jnp.float32)
    for index in range(N_MP):
        part = lax.dot_general(query_masked[:, index * query_cols:(index + 1) * query_cols],
                               query_projection_weight[:, index * query_cols:(index + 1) * query_cols],
                               (((1,), (1,)), ((), ())), preferred_element_type=jnp.float32)
        hidden_total_sum = hidden_total_sum + lax.optimization_barrier(part.astype(jnp.bfloat16)).astype(jnp.float32)
        other = lax.dot_general(output_masked[:, index * output_cols:(index + 1) * output_cols],
                                output_projection_weight[:, index * output_cols:(index + 1) * output_cols],
                                (((1,), (1,)), ((), ())), preferred_element_type=jnp.float32)
        attended_total_sum = attended_total_sum + lax.optimization_barrier(other.astype(jnp.bfloat16)).astype(jnp.float32)
    hidden_state_gradient = (hidden_total_sum + hidden_adapter_term.astype(jnp.float32)).astype(jnp.bfloat16)
    attention_output_gradient = (attended_total_sum + attended_adapter_term.astype(jnp.float32)).astype(jnp.bfloat16)
    return (queries, projected, hidden_state_gradient, attention_output_gradient,
            narrower_gradient, widener_gradient, reducer_gradient, enlarger_gradient)
```

```python
import jax
import jax.numpy as jnp
from jax import lax
from jax.experimental import pallas as pl
from jax.experimental.pallas import tpu as pltpu
from jax.sharding import Mesh
from jax.sharding import PartitionSpec as P

adapter_scale = 2.0
F32 = jnp.float32
BF16 = jnp.bfloat16
DP = ("y", "z")
MP = ("x", "c")


def matmul(left, right, ldim=1, rdim=0):
    return lax.dot_general(
        left, right, (((ldim,), (rdim,)), ((), ())), preferred_element_type=F32
    )


def iota(shape, dim):
    return lax.broadcasted_iota(jnp.int32, shape, dim)


def forward_kernel(order_ref, *refs):
    row_refs, (w_ref, keep_ref, give_ref, total) = refs[:-4], refs[-4:]
    step = pl.program_id(0)
    sides, tokens, width = keep_ref.shape

    @pl.when(step == 0)
    def _():
        total[...] = jnp.zeros_like(total)

    for k, rows_ref in enumerate(row_refs):

        @pl.when(step == k)
        def _():
            for w in range(sides):
                rows = jnp.concatenate([rows_ref[0, w], rows_ref[1, w]], axis=0)
                total[w] += jnp.dot(
                    rows, w_ref[0, :, w * width : (w + 1) * width], preferred_element_type=F32
                )

    @pl.when(step == pl.num_programs(0) - 1)
    def _():
        keep_ref[...] = total[:, :tokens]
        give_ref[...] = total[:, tokens:].astype(BF16)


def forward_base(order, rows, weights):
    steps, depth, wide = weights.shape
    _, sides, tokens, _ = rows[0].shape
    width = wide // sides
    whole = pl.BlockSpec(rows[0].shape, lambda k, order: (0, 0, 0, 0))
    out = pl.BlockSpec((sides, tokens, width), lambda k, order: (0, 0, 0))
    return pl.pallas_call(
        forward_kernel,
        grid_spec=pltpu.PrefetchScalarGridSpec(
            num_scalar_prefetch=1,
            grid=(steps,),
            in_specs=[whole] * steps
            + [pl.BlockSpec((1, depth, wide), lambda k, order: (order[k], 0, 0))],
            out_specs=[out, out],
            scratch_shapes=[pltpu.VMEM((sides, 2 * tokens, width), F32)],
        ),
        out_shape=[
            jax.ShapeDtypeStruct((sides, tokens, width), F32),
            jax.ShapeDtypeStruct((sides, tokens, width), BF16),
        ],
        compiler_params=pltpu.CompilerParams(dimension_semantics=("arbitrary",)),
        cost_estimate=pl.CostEstimate(
            flops=4 * tokens * steps * depth * wide,
            bytes_accessed=weights.size * 2 + 2 * steps * rows[0].size,
            transcendentals=0,
        ),
        name="forward_base",
    )(order, *rows, weights)


def backward_kernel(first_ref, own_ref, other_ref, w_ref, out_ref, part):
    sides, tokens, width = own_ref.shape
    for w in range(sides):
        rows = jnp.concatenate([own_ref[w], other_ref[w]], axis=0)
        part[w] = lax.dot_general(
            rows,
            w_ref[0, :, w * width : (w + 1) * width],
            (((1,), (1,)), ((), ())),
            preferred_element_type=F32,
        )
    own_first = first_ref[0] == 0

    @pl.when(own_first)
    def _():
        out_ref[0, 0] = part[:, :tokens].astype(BF16)
        out_ref[0, 1] = part[:, tokens:].astype(BF16)

    @pl.when(jnp.logical_not(own_first))
    def _():
        out_ref[0, 0] = part[:, tokens:].astype(BF16)
        out_ref[0, 1] = part[:, :tokens].astype(BF16)


def backward_base(first, own, other, weights):
    steps, depth, wide = weights.shape
    sides, tokens, _ = own.shape
    width = wide // sides
    rows = pl.BlockSpec((sides, tokens, width), lambda k, first: (0, 0, 1))
    out = pl.BlockSpec((1, 2, sides, tokens, depth), lambda k, first: (k, 0, 0, 0, 0))
    return pl.pallas_call(
        backward_kernel,
        grid_spec=pltpu.PrefetchScalarGridSpec(
            num_scalar_prefetch=1,
            grid=(steps,),
            in_specs=[rows, rows, pl.BlockSpec((1, depth, wide), lambda k, first: (k, 0, 0))],
            out_specs=out,
            scratch_shapes=[pltpu.VMEM((sides, 2 * tokens, depth), F32)],
        ),
        out_shape=jax.ShapeDtypeStruct((steps, 2, sides, tokens, depth), BF16),
        compiler_params=pltpu.CompilerParams(dimension_semantics=("arbitrary",)),
        cost_estimate=pl.CostEstimate(
            flops=4 * tokens * steps * depth * wide,
            bytes_accessed=weights.size * 2 + 4 * steps * sides * tokens * depth,
            transcendentals=0,
        ),
        name="backward_base",
    )(first, own, other, weights)


def on_device(
    hidden,
    attended,
    query_cotangent,
    output_cotangent,
    query_projection_weight,
    output_projection_weight,
    narrower,
    widener,
    reducer,
    enlarger,
    block_adapter,
    block_fill,
):
    tokens, width = hidden.shape
    blocks = block_adapter.shape[0]
    rows = tokens // blocks
    ny, nx, nc = lax.axis_size("y"), lax.axis_size("x"), lax.axis_size("c")
    owners = ny * lax.axis_size("z")
    mine, rank = narrower.shape[:2]
    y, x, c = lax.axis_index("y"), lax.axis_index("x"), lax.axis_index("c")
    odd = y % 2
    neighbour = [(i, i ^ 1) for i in range(ny)]

    weights = jnp.concatenate([query_projection_weight, output_projection_weight], axis=1)
    same_parity = [[p + 2 * i for i in range(ny // 2)] for p in range(2)]
    weights = lax.all_gather(weights, "y", axis=0, axis_index_groups=same_parity)
    weights = lax.all_gather(weights, "z", axis=1, tiled=True)

    owner_of = (block_adapter // mine).astype(BF16)
    local_of = block_adapter % mine
    fill = block_fill.astype(BF16)
    in_block = (iota((tokens, blocks), 0) // rows == iota((tokens, blocks), 1)).astype(BF16)
    local_hot = (iota((blocks, 128), 1) == local_of[:, None]).astype(BF16)
    token_local = matmul(in_block, local_hot).astype(BF16)
    token_fill = matmul(in_block, jnp.broadcast_to(fill[:, None], (blocks, 128)))[:, :1]
    live = (iota((tokens, 1), 0) % rows < token_fill.astype(jnp.int32)).astype(BF16)
    token_owner = matmul(jnp.broadcast_to(owner_of[None, :], (8, blocks)), in_block, 1, 1)[:1]
    token_owner = token_owner.astype(jnp.int32)
    both = 2 * tokens
    slot_rows = owners * 2 * rows
    table_owner = jnp.concatenate([token_owner, token_owner], axis=1)
    table_row = iota((slot_rows, both), 0)
    table_col = iota((slot_rows, both), 1)
    table = (
        (table_row // (2 * rows) == table_owner)
        & (table_row % rows == table_col % rows)
        & ((table_row // rows) % 2 == table_col // tokens)
    ).astype(BF16)

    inputs = jnp.concatenate([hidden, attended], axis=0)
    cotangents = jnp.concatenate([query_cotangent * live, output_cotangent * live], axis=0)

    tags = jnp.concatenate([token_local, token_local], axis=0)
    payload = jnp.concatenate([inputs, cotangents, tags], axis=1)

    other = lax.ppermute(payload, "y", neighbour)
    at_home = c == odd
    hand_over = [(a * nc + a % 2, a * nc + 1 - a % 2) for a in range(ny)]
    trade = [
        (a * nc + b, ((a ^ 1) * nc + (b ^ 1)) if a % 2 != b else a * nc + b)
        for a in range(ny)
        for b in range(nc)
    ]
    features = jnp.concatenate([payload[:, :width], other[:, :width]], axis=0)
    features = jnp.where(at_home, features, lax.ppermute(features, ("y", "c"), hand_over))
    shifts = (0, 1, nx - 1, 2)
    order = jnp.stack([(x + nx - k) % nx for k in shifts]).astype(jnp.int32)
    gathered = [features]
    for k in shifts[1:]:
        ring = [(i, (i + k) % nx) for i in range(nx)]
        gathered.append(lax.ppermute(features, "x", ring))
    features = [f.reshape(2, 2, tokens, width) for f in gathered]

    send = matmul(table, payload).astype(BF16).reshape(owners, 2 * rows, payload.shape[1])
    recv = lax.all_to_all(send, DP, 0, 0, tiled=True).reshape(slot_rows, payload.shape[1])
    slot_inputs = recv[:, :width]
    slot_cotangents = recv[:, width : 2 * width]
    slot_tags = recv[:, 2 * width :]
    lanes = 2 * mine * rank
    half = mine * rank
    spread = (iota((128, lanes), 0) == (iota((128, lanes), 1) % half) // rank).astype(BF16)
    side = (iota((slot_rows, lanes), 0) // rows) % 2 == iota((slot_rows, lanes), 1) // half
    mask = matmul(slot_tags, spread).astype(BF16) * side.astype(BF16)
    fold = (iota((lanes, rank), 0) % rank == iota((lanes, rank), 1)).astype(BF16)
    down = jnp.concatenate([narrower.reshape(half, width), reducer.reshape(half, width)], axis=0)
    up = jnp.concatenate([widener.reshape(half, width), enlarger.reshape(half, width)], axis=0)
    forward_wide = matmul(slot_inputs, down, 1, 1).astype(BF16) * mask
    backward_wide = matmul(slot_cotangents, up, 1, 1).astype(BF16) * mask
    forward_part = matmul(fold, forward_wide, 0, 1).astype(BF16)
    backward_part = matmul(fold, backward_wide, 0, 1).astype(BF16)
    parts = jnp.concatenate([forward_part, backward_part], axis=0)
    shares = lax.axis_size(MP)
    copies = jnp.broadcast_to(parts, (shares, *parts.shape))
    everyone = lax.all_to_all(copies, MP, 0, 0, tiled=True)
    ranks = jnp.sum(everyone.astype(F32), axis=0).astype(BF16)
    forward_ranks = matmul(ranks[:rank], fold, 0, 1).astype(BF16) * mask
    backward_ranks = matmul(ranks[rank:], fold, 0, 1).astype(BF16) * mask
    raised = jnp.concatenate(
        [
            (adapter_scale * matmul(forward_ranks, up)).astype(BF16),
            (adapter_scale * matmul(backward_ranks, down)).astype(BF16),
        ],
        axis=1,
    )

    def gradient(left, right):
        return (adapter_scale * matmul(left, right, 0, 0)).reshape(mine, rank, width)

    narrower_gradient = gradient(backward_ranks[:, :half], slot_inputs)
    reducer_gradient = gradient(backward_ranks[:, half:], slot_inputs)
    widener_gradient = gradient(forward_ranks[:, :half], slot_cotangents)
    enlarger_gradient = gradient(forward_ranks[:, half:], slot_cotangents)

    gradients = (narrower_gradient, widener_gradient, reducer_gradient, enlarger_gradient)
    raised = raised.reshape(owners, 2 * rows, 2 * width)
    gradients, weights = lax.optimization_barrier((gradients, weights))

    wide = payload.shape[1]
    chunks = backward_base(
        odd.astype(jnp.int32).reshape(1),
        payload.reshape(2, tokens, wide),
        other.reshape(2, tokens, wide),
        weights,
    )
    chunks = chunks.reshape(nx * nc, both, width)
    raised, chunks = lax.optimization_barrier((raised, chunks))
    total = lax.psum_scatter(chunks, MP, scatter_dimension=0, tiled=False)
    total = lax.ppermute(total, ("y", "c"), trade).astype(F32)
    back = lax.all_to_all(
        raised, DP, 0, 0, tiled=True
    ).reshape(slot_rows, 2 * width)
    terms = matmul(table, back, 0, 0)

    keep, give = forward_base(order, features, weights)
    keep = keep.reshape(both, width)
    keep = keep + lax.ppermute(give.reshape(both, width), "y", neighbour).astype(F32)

    forward_out = (keep + terms[:, :width]).astype(BF16)
    backward_out = (total.astype(BF16).astype(F32) + terms[:, width:]).astype(BF16)
    return (
        forward_out[:tokens],
        forward_out[tokens:],
        backward_out[:tokens],
        backward_out[tokens:],
        *gradients,
    )


def solution(mesh):
    grid = Mesh(mesh.devices.reshape(8, 8, 4, 2), ("y", "z", "x", "c"))
    flat = P(DP, MP)
    deep = P(DP, None, MP)

    return jax.shard_map(
        on_device,
        mesh=grid,
        in_specs=(flat,) * 6 + (deep,) * 4 + (P(DP),) * 2,
        out_specs=(flat,) * 4 + (deep,) * 4,
        check_vma=False,
    )
```

```python
import jax
import jax.numpy as jnp
from jax import lax
from jax.experimental import pallas as pl
from jax.experimental.pallas import tpu as pltpu
from jax.sharding import Mesh
from jax.sharding import PartitionSpec as P

adapter_scale = 2.0
F32 = jnp.float32
BF16 = jnp.bfloat16
DP = ("y", "z")
MP = ("x", "c")


def matmul(left, right, ldim=1, rdim=0):
    return lax.dot_general(
        left, right, (((ldim,), (rdim,)), ((), ())), preferred_element_type=F32
    )


def iota(shape, dim):
    return lax.broadcasted_iota(jnp.int32, shape, dim)


def forward_kernel(order_ref, *refs):
    row_refs, (w_ref, keep_ref, give_ref, total) = refs[:-4], refs[-4:]
    step = pl.program_id(0)
    sides, tokens, width = keep_ref.shape

    @pl.when(step == 0)
    def _():
        total[...] = jnp.zeros_like(total)

    for k, rows_ref in enumerate(row_refs):

        @pl.when(step == k)
        def _():
            for w in range(sides):
                rows = jnp.concatenate([rows_ref[0, w], rows_ref[1, w]], axis=0)
                total[w] += jnp.dot(
                    rows, w_ref[0, :, w * width : (w + 1) * width], preferred_element_type=F32
                )

    @pl.when(step == pl.num_programs(0) - 1)
    def _():
        keep_ref[...] = total[:, :tokens]
        give_ref[...] = total[:, tokens:].astype(BF16)


def forward_base(order, rows, weights):
    steps, depth, wide = weights.shape
    _, sides, tokens, _ = rows[0].shape
    width = wide // sides
    whole = pl.BlockSpec(rows[0].shape, lambda k, order: (0, 0, 0, 0))
    out = pl.BlockSpec((sides, tokens, width), lambda k, order: (0, 0, 0))
    return pl.pallas_call(
        forward_kernel,
        grid_spec=pltpu.PrefetchScalarGridSpec(
            num_scalar_prefetch=1,
            grid=(steps,),
            in_specs=[whole] * steps
            + [pl.BlockSpec((1, depth, wide), lambda k, order: (order[k], 0, 0))],
            out_specs=[out, out],
            scratch_shapes=[pltpu.VMEM((sides, 2 * tokens, width), F32)],
        ),
        out_shape=[
            jax.ShapeDtypeStruct((sides, tokens, width), F32),
            jax.ShapeDtypeStruct((sides, tokens, width), BF16),
        ],
        compiler_params=pltpu.CompilerParams(dimension_semantics=("arbitrary",)),
        cost_estimate=pl.CostEstimate(
            flops=4 * tokens * steps * depth * wide,
            bytes_accessed=weights.size * 2 + 2 * steps * rows[0].size,
            transcendentals=0,
        ),
        name="forward_base",
    )(order, *rows, weights)


def backward_kernel(first_ref, own_ref, other_ref, w_ref, kept_ref, sent_ref, part):
    sides, tokens, width = own_ref.shape
    for w in range(sides):
        rows = jnp.concatenate([own_ref[w], other_ref[w]], axis=0)
        part[w] = lax.dot_general(
            rows,
            w_ref[0, :, w * width : (w + 1) * width],
            (((1,), (1,)), ((), ())),
            preferred_element_type=F32,
        )
    own_first = first_ref[0] == 0

    @pl.when(own_first)
    def _():
        kept_ref[0] = part[:, :tokens].astype(BF16)
        sent_ref[0] = part[:, tokens:].astype(BF16)

    @pl.when(jnp.logical_not(own_first))
    def _():
        kept_ref[0] = part[:, tokens:].astype(BF16)
        sent_ref[0] = part[:, :tokens].astype(BF16)


def backward_base(first, own, other, weights):
    steps, depth, wide = weights.shape
    sides, tokens, _ = own.shape
    width = wide // sides
    rows = pl.BlockSpec((sides, tokens, width), lambda k, first: (0, 0, 1))
    out = pl.BlockSpec((1, sides, tokens, depth), lambda k, first: (k, 0, 0, 0))
    return pl.pallas_call(
        backward_kernel,
        grid_spec=pltpu.PrefetchScalarGridSpec(
            num_scalar_prefetch=1,
            grid=(steps,),
            in_specs=[rows, rows, pl.BlockSpec((1, depth, wide), lambda k, first: (k, 0, 0))],
            out_specs=[out, out],
            scratch_shapes=[pltpu.VMEM((sides, 2 * tokens, depth), F32)],
        ),
        out_shape=[jax.ShapeDtypeStruct((steps, sides, tokens, depth), BF16)] * 2,
        compiler_params=pltpu.CompilerParams(dimension_semantics=("arbitrary",)),
        cost_estimate=pl.CostEstimate(
            flops=4 * tokens * steps * depth * wide,
            bytes_accessed=weights.size * 2 + 4 * steps * sides * tokens * depth,
            transcendentals=0,
        ),
        name="backward_base",
    )(first, own, other, weights)


def on_device(
    hidden,
    attended,
    query_cotangent,
    output_cotangent,
    query_projection_weight,
    output_projection_weight,
    narrower,
    widener,
    reducer,
    enlarger,
    block_adapter,
    block_fill,
):
    tokens, width = hidden.shape
    blocks = block_adapter.shape[0]
    rows = tokens // blocks
    ny, nx, nc = lax.axis_size("y"), lax.axis_size("x"), lax.axis_size("c")
    owners = ny * lax.axis_size("z")
    mine, rank = narrower.shape[:2]
    y, x, c = lax.axis_index("y"), lax.axis_index("x"), lax.axis_index("c")
    odd = y % 2
    neighbour = [(i, i ^ 1) for i in range(ny)]

    weights = jnp.concatenate([query_projection_weight, output_projection_weight], axis=1)
    same_parity = [[p + 2 * i for i in range(ny // 2)] for p in range(2)]
    weights = lax.all_gather(weights, "y", axis=0, axis_index_groups=same_parity)
    weights = lax.all_gather(weights, "z", axis=1, tiled=True)

    owner_of = (block_adapter // mine).astype(BF16)
    local_of = block_adapter % mine
    fill = block_fill.astype(BF16)
    in_block = (iota((tokens, blocks), 0) // rows == iota((tokens, blocks), 1)).astype(BF16)
    local_hot = (iota((blocks, 128), 1) == local_of[:, None]).astype(BF16)
    token_local = matmul(in_block, local_hot).astype(BF16)
    token_fill = matmul(in_block, jnp.broadcast_to(fill[:, None], (blocks, 128)))[:, :1]
    live = (iota((tokens, 1), 0) % rows < token_fill.astype(jnp.int32)).astype(BF16)
    token_owner = matmul(jnp.broadcast_to(owner_of[None, :], (8, blocks)), in_block, 1, 1)[:1]
    token_owner = token_owner.astype(jnp.int32)
    both = 2 * tokens
    slot_rows = owners * 2 * rows
    table_owner = jnp.concatenate([token_owner, token_owner], axis=1)
    table_row = iota((slot_rows, both), 0)
    table_col = iota((slot_rows, both), 1)
    table = (
        (table_row // (2 * rows) == table_owner)
        & (table_row % rows == table_col % rows)
        & ((table_row // rows) % 2 == table_col // tokens)
    ).astype(BF16)

    inputs = jnp.concatenate([hidden, attended], axis=0)
    cotangents = jnp.concatenate([query_cotangent * live, output_cotangent * live], axis=0)

    tags = jnp.concatenate([token_local, token_local], axis=0)
    payload = jnp.concatenate([inputs, cotangents, tags], axis=1)

    other = lax.ppermute(payload, "y", neighbour)
    at_home = c == odd
    hand_over = [(a * nc + a % 2, a * nc + 1 - a % 2) for a in range(ny)]
    trade = [
        (a * nc + b, ((a ^ 1) * nc + (b ^ 1)) if a % 2 != b else a * nc + b)
        for a in range(ny)
        for b in range(nc)
    ]
    features = jnp.concatenate([payload[:, :width], other[:, :width]], axis=0)
    features = jnp.where(at_home, features, lax.ppermute(features, ("y", "c"), hand_over))
    shifts = (0, 1, nx - 1, 2)
    order = jnp.stack([(x + nx - k) % nx for k in shifts]).astype(jnp.int32)
    gathered = [features]
    for k in shifts[1:]:
        ring = [(i, (i + k) % nx) for i in range(nx)]
        gathered.append(lax.ppermute(features, "x", ring))
    features = [f.reshape(2, 2, tokens, width) for f in gathered]

    send = matmul(table, payload).astype(BF16).reshape(owners, 2 * rows, payload.shape[1])
    recv = lax.all_to_all(send, DP, 0, 0, tiled=True).reshape(slot_rows, payload.shape[1])
    slot_inputs = recv[:, :width]
    slot_cotangents = recv[:, width : 2 * width]
    slot_tags = recv[:, 2 * width :]
    lanes = 2 * mine * rank
    half = mine * rank
    spread = (iota((128, lanes), 0) == (iota((128, lanes), 1) % half) // rank).astype(BF16)
    side = (iota((slot_rows, lanes), 0) // rows) % 2 == iota((slot_rows, lanes), 1) // half
    mask = matmul(slot_tags, spread).astype(BF16) * side.astype(BF16)
    fold = (iota((lanes, rank), 0) % rank == iota((lanes, rank), 1)).astype(BF16)
    down = jnp.concatenate([narrower.reshape(half, width), reducer.reshape(half, width)], axis=0)
    up = jnp.concatenate([widener.reshape(half, width), enlarger.reshape(half, width)], axis=0)
    forward_wide = matmul(slot_inputs, down, 1, 1).astype(BF16) * mask
    backward_wide = matmul(slot_cotangents, up, 1, 1).astype(BF16) * mask
    forward_part = matmul(fold, forward_wide, 0, 1).astype(BF16)
    backward_part = matmul(fold, backward_wide, 0, 1).astype(BF16)
    parts = jnp.concatenate([forward_part, backward_part], axis=0)
    shares = lax.axis_size(MP)
    copies = jnp.broadcast_to(parts, (shares, *parts.shape))
    everyone = lax.all_to_all(copies, MP, 0, 0, tiled=True)
    ranks = jnp.sum(everyone.astype(F32), axis=0).astype(BF16)
    forward_ranks = matmul(ranks[:rank], fold, 0, 1).astype(BF16) * mask
    backward_ranks = matmul(ranks[rank:], fold, 0, 1).astype(BF16) * mask
    raised = jnp.concatenate(
        [
            (adapter_scale * matmul(forward_ranks, up)).astype(BF16),
            (adapter_scale * matmul(backward_ranks, down)).astype(BF16),
        ],
        axis=1,
    )

    def gradient(left, right):
        return (adapter_scale * matmul(left, right, 0, 0)).reshape(mine, rank, width)

    narrower_gradient = gradient(backward_ranks[:, :half], slot_inputs)
    reducer_gradient = gradient(backward_ranks[:, half:], slot_inputs)
    widener_gradient = gradient(forward_ranks[:, :half], slot_cotangents)
    enlarger_gradient = gradient(forward_ranks[:, half:], slot_cotangents)

    gradients = (narrower_gradient, widener_gradient, reducer_gradient, enlarger_gradient)
    raised = raised.reshape(owners, 2 * rows, 2 * width)
    gradients, raised = lax.optimization_barrier((gradients, raised))
    back = lax.all_to_all(
        raised, DP, 0, 0, tiled=True
    ).reshape(slot_rows, 2 * width)
    terms = matmul(table, back, 0, 0)

    wide = payload.shape[1]
    kept, sent = backward_base(
        (c ^ odd).astype(jnp.int32).reshape(1),
        payload.reshape(2, tokens, wide),
        other.reshape(2, tokens, wide),
        weights,
    )
    kept = kept.reshape(nx, both, width)
    sent = sent.reshape(nx, both, width)
    got = lax.ppermute(sent, "c", [(0, 1), (1, 0)])

    pair = (kept.astype(F32) + got.astype(F32)).astype(BF16)
    total = lax.psum_scatter(pair, "x", scatter_dimension=0, tiled=False)
    total = lax.ppermute(total, ("y", "c"), trade).astype(F32)

    keep, give = forward_base(order, features, weights)
    keep = keep.reshape(both, width)
    keep = keep + lax.ppermute(give.reshape(both, width), "y", neighbour).astype(F32)

    forward_out = (keep + terms[:, :width]).astype(BF16)
    backward_out = (total.astype(BF16).astype(F32) + terms[:, width:]).astype(BF16)
    return (
        forward_out[:tokens],
        forward_out[tokens:],
        backward_out[:tokens],
        backward_out[tokens:],
        *gradients,
    )


def solution(mesh):
    grid = Mesh(mesh.devices.reshape(8, 8, 4, 2), ("y", "z", "x", "c"))
    flat = P(DP, MP)
    deep = P(DP, None, MP)

    return jax.shard_map(
        on_device,
        mesh=grid,
        in_specs=(flat,) * 6 + (deep,) * 4 + (P(DP),) * 2,
        out_specs=(flat,) * 4 + (deep,) * 4,
        check_vma=False,
    )
```
